32 devices in a mesh: row: 4 (over x, core), col: 8 (over z, y).
Axes of the slice: x: 2, y: 2, z: 4, core: 2. Of those that a mesh axis runs over, the one named last changes fastest.
Arguments:
- stem: float32 [2, 4, 1024, 1024], P(None, 'row', 'col'), may hold values from -6 to 6
- branch: float32 [2, 1024, 1024], replicated, may hold values from -0.125 to 0.125
Outputs:
- absorbed: float32 [2, 1024, 4, 1024], P(None, ('row', 'col'))
The draws below stay inside these ranges and needn't reach their ends.
All inputs are finite; a program needn't handle non-finite values.
Results may differ from the reference program's by a relative error of at most 0.00007.
Values sent between devices are 32-bit elements; how exact they have to be, the bound alone decides.
No kernel may reach another device: no remote copies, remote signals or barrier semaphores. Data moves between devices by JAX's collectives and lax.ppermute only.
A program may use at most 64 MiB of HBM per device.

```python
import jax
import jax.numpy as jnp
from jax import lax

CONTRACT = 1024
OPENED = 1024
LOCAL = 1024
GROUP_A = 4
GROUP_B = 1024
MIDDLE = 1


def steps_of(own_key, extent, cuts, least, high):
    def one(dim, blocks):
        draws = jax.random.uniform(jax.random.fold_in(jax.random.fold_in(own_key, 6), dim), (blocks,), jnp.float32, least / len(cuts), high / len(cuts))
        return jnp.repeat(jnp.exp(draws), extent[dim] // blocks).reshape((-1,) + (1,) * (len(extent) - dim - 1))

    factor_of = one(*cuts[0])
    for cut in cuts[1:]:
        factor_of = factor_of * one(*cut)
    return factor_of


def noise(rng, dims, scale, bound, pieces=(), dtype=jnp.bfloat16):
    drawn = scale * jax.random.normal(rng, dims, jnp.float32)
    if pieces:
        drawn = drawn * steps_of(rng, dims, pieces, -0.22, 0.18)
    return jnp.clip(drawn, -bound, bound).astype(dtype)


def setup_inputs(seed: int = 0) -> dict:
    arg_keys = jax.random.split(jax.random.key(seed), 3)
    return {
        "stem": noise(arg_keys[0], (2, GROUP_A, GROUP_B, LOCAL), 1.0, 6.0, ((1, 4), (2, 8)), jnp.float32),
        "branch": noise(arg_keys[1], (2, CONTRACT, OPENED), (2 * CONTRACT) ** -0.5, 0.125, (), jnp.float32),
    }


def reference(stem, branch):
    split = stem.reshape(2, GROUP_A, CONTRACT, MIDDLE, LOCAL)
    high = lax.Precision.HIGHEST
    real = jnp.einsum("akml,ko->lamo", split[0], branch[0], precision=high) - jnp.einsum("akml,ko->lamo", split[1], branch[1], precision=high)
    imag = jnp.einsum("akml,ko->lamo", split[0], branch[1], precision=high) + jnp.einsum("akml,ko->lamo", split[1], branch[0], precision=high)
    joined = jnp.stack([real, imag]).astype(jnp.float32)
    return joined.reshape(2, LOCAL, GROUP_A, MIDDLE * OPENED)
```

```python
import functools

import jax
import jax.numpy as jnp
from jax import lax
from jax.experimental import pallas as pl
from jax.experimental.pallas import tpu as pltpu
from jax.sharding import PartitionSpec as P

LANES = 128
SUBLANES = 8


def plain(stem, branch):
    rows_count = lax.axis_size("row")
    cols_count = lax.axis_size("col")
    entries = stem.shape[2]
    remain = stem.shape[3]
    contract = branch.shape[1]
    opened = branch.shape[2]
    middle = entries * cols_count // contract
    owned = remain // (rows_count * cols_count)
    blocks = stem.reshape(2, 1, entries, rows_count * cols_count, owned)
    blocks = jnp.moveaxis(blocks, 3, 0)
    moved = lax.all_to_all(blocks, ("row", "col"), 0, 0, tiled=True)
    moved = moved.reshape(rows_count, cols_count, 2, entries, owned)
    split = moved.transpose(2, 0, 1, 3, 4).reshape(
        2, rows_count, contract, middle, owned
    )
    high = lax.Precision.HIGHEST
    dot = functools.partial(jnp.einsum, "akml,ko->lamo", precision=high)
    real = dot(split[0], branch[0]) - dot(split[1], branch[1])
    imag = dot(split[0], branch[1]) + dot(split[1], branch[0])
    return jnp.stack([real, imag]).reshape(2, owned, rows_count, middle * opened)


def pack_kernel(stem_ref, out_ref):
    blocks, _, owned, entries = out_ref.shape
    for c in range(2):
        turned = stem_ref[c, 0].T
        out_ref[:, c] = turned.reshape(blocks, owned, entries)


def pack(stem, owned, steps):
    _, _, entries, remain = stem.shape
    width = remain // steps
    return pl.pallas_call(
        pack_kernel,
        grid=(steps,),
        in_specs=[pl.BlockSpec((2, 1, entries, width), lambda i: (0, 0, 0, i))],
        out_specs=pl.BlockSpec(
            (width // owned, 2, owned, entries), lambda i: (i, 0, 0, 0)
        ),
        out_shape=jax.ShapeDtypeStruct(
            (remain // owned, 2, owned, entries), jnp.float32
        ),
        name="pack",
    )(stem)


def halves(x):
    high = x.astype(jnp.bfloat16)
    low = (x - high.astype(jnp.float32)).astype(jnp.bfloat16)
    return high, low


def absorb_kernel(rows_count, moved_ref, branch_ref, out_ref, gathered, high, low):
    blocks, _, owned, entries = moved_ref.shape
    cols_count = blocks // rows_count
    rows = rows_count * owned

    @pl.when(pl.program_id(0) == 0)
    def _():
        for c in range(2):
            for j in range(cols_count):
                for a in range(rows_count):
                    gathered[pl.ds(c * rows + a, owned, stride=rows_count), :] = (
                        moved_ref[a * cols_count + j, c]
                    )
                at = pl.ds(c * rows, rows)
                cols = pl.ds(j * entries, entries)
                high[at, cols], low[at, cols] = halves(gathered[at, :])

    dot = functools.partial(jnp.dot, preferred_element_type=jnp.float32)

    def product(part):
        branch_high, branch_low = halves(branch_ref[part])
        return (
            dot(high[...], branch_low) + dot(low[...], branch_high)
        ) + dot(high[...], branch_high)

    with_real = product(0)
    with_imag = product(1)
    width = out_ref.shape[-1]
    real = with_real[:rows] - with_imag[rows:]
    imag = with_imag[:rows] + with_real[rows:]
    out_ref[0] = real.reshape(owned, rows_count, width)
    out_ref[1] = imag.reshape(owned, rows_count, width)


def absorb(moved, branch, rows_count, steps):
    blocks, _, owned, entries = moved.shape
    _, contract, opened = branch.shape
    width = opened // steps
    rows = 2 * owned * rows_count
    return pl.pallas_call(
        functools.partial(absorb_kernel, rows_count),
        grid=(steps,),
        in_specs=[
            pl.BlockSpec(moved.shape, lambda i: (0, 0, 0, 0)),
            pl.BlockSpec((2, contract, width), lambda i: (0, 0, i)),
        ],
        out_specs=pl.BlockSpec((2, owned, rows_count, width), lambda i: (0, 0, 0, i)),
        out_shape=jax.ShapeDtypeStruct((2, owned, rows_count, opened), jnp.float32),
        scratch_shapes=[
            pltpu.VMEM((rows, entries), jnp.float32),
            pltpu.VMEM((rows, contract), jnp.bfloat16),
            pltpu.VMEM((rows, contract), jnp.bfloat16),
        ],
        name="absorb",
    )(moved, branch)


def per_device(stem, branch):
    rows_count = lax.axis_size("row")
    cols_count = lax.axis_size("col")
    _, _, entries, remain = stem.shape
    _, contract, opened = branch.shape
    owned = remain // (rows_count * cols_count)
    fits = (
        entries * cols_count == contract
        and entries % LANES == 0
        and owned % SUBLANES == 0
        and opened % (4 * LANES) == 0
        and remain % (4 * LANES) == 0
    )
    if not fits:
        return plain(stem, branch)
    packed = pack(stem, owned, 4)
    moved = lax.all_to_all(packed, ("row", "col"), 0, 0, tiled=True)
    return absorb(moved, branch, rows_count, 4)


def solution(mesh):
    placed = (P(None, "row", "col", None), P())
    return jax.shard_map(
        per_device,
        mesh=mesh,
        in_specs=placed,
        out_specs=P(None, ("row", "col"), None, None),
        check_vma=False,
    )
```

```python
import functools

import jax
import jax.numpy as jnp
from jax import lax
from jax.experimental import pallas as pl
from jax.experimental.pallas import tpu as pltpu
from jax.sharding import Mesh, PartitionSpec as P


LANES = 128
SUBLANES = 8
STEPS = 4


COLS = ("far", "near", "side")
PLANE = ("row", "side")


def counts():
    rows_count = lax.axis_size("row")
    cols_count = 1
    for name in COLS:
        cols_count *= lax.axis_size(name)
    return rows_count, cols_count


def plain(stem, branch):
    rows_count, cols_count = counts()
    entries = stem.shape[2]
    remain = stem.shape[3]
    contract = branch.shape[1]
    opened = branch.shape[2]
    middle = entries * cols_count // contract
    owned = remain // (rows_count * cols_count)
    blocks = stem.reshape(2, 1, entries, rows_count * cols_count, owned)
    blocks = jnp.moveaxis(blocks, 3, 0)
    moved = lax.all_to_all(blocks, ("row", *COLS), 0, 0, tiled=True)
    moved = moved.reshape(rows_count, cols_count, 2, entries, owned)
    split = moved.transpose(2, 0, 1, 3, 4).reshape(
        2, rows_count, contract, middle, owned
    )
    high = lax.Precision.HIGHEST
    dot = functools.partial(jnp.einsum, "akml,ko->lamo", precision=high)
    real = dot(split[0], branch[0]) - dot(split[1], branch[1])
    imag = dot(split[0], branch[1]) + dot(split[1], branch[0])
    return jnp.stack([real, imag]).reshape(2, owned, rows_count, middle * opened)


def params(mib):
    return pltpu.CompilerParams(vmem_limit_bytes=mib << 20)


def whole():
    return pl.BlockSpec(memory_space=pltpu.VMEM)


def turned(stem_ref, r, c, width, far):
    start = pl.multiple_of((2 * r + far) * width, width)
    return stem_ref[c, 0, :, pl.ds(start, width)].T


def place(stem_ref, far, same, other):
    entries = stem_ref.shape[2]
    blocks, _, owned, _ = same.shape
    rows_count = lax.axis_size("row")
    sides = blocks // rows_count
    half = sides * owned
    here = lax.axis_index("near") == 0
    for r in range(rows_count):
        at = pl.ds(r * sides, sides)
        for c in range(2):
            whole_width = turned(stem_ref, r, c, 2 * half, far)
            low, high = whole_width[:half], whole_width[half:]
            shape = (sides, owned, entries)
            same[at, c] = jnp.where(here, low, high).reshape(shape)
            other[at, c] = jnp.where(here, high, low).reshape(shape)


def pack_far_kernel(stem_ref, first_ref, second_ref):
    place(stem_ref, 1 - lax.axis_index("far"), first_ref, second_ref)


def pack_near_kernel(stem_ref, second_ref, early_ref, beside_ref):
    early_ref[:, 0] = second_ref[...]
    place(stem_ref, lax.axis_index("far"), early_ref.at[:, 1], beside_ref)


def part_of_kernel(early_ref, second_ref):
    second_ref[...] = early_ref[:, 0]


def join_kernel(first_ref, beside_ref, late_ref):
    late_ref[:, 0] = first_ref[...]
    late_ref[:, 1] = beside_ref[...]


def small(kernel, args, outs):
    return pl.pallas_call(
        kernel,
        in_specs=[whole()] * len(args),
        out_specs=[whole()] * len(outs),
        out_shape=[jax.ShapeDtypeStruct(out, jnp.float32) for out in outs],
        compiler_params=params(4),
    )(*args)


def halves(x):
    high = x.astype(jnp.bfloat16)
    low = (x - high.astype(jnp.float32)).astype(jnp.bfloat16)
    return high, low


def gather(moved_ref, which, gathered, both):
    blocks, _, _, owned, entries = moved_ref.shape
    rows = both.shape[0] // 4
    rows_count = rows // owned
    sides = blocks // rows_count
    for j in range(sides):
        for c in range(2):
            for r in range(rows_count):
                gathered[pl.ds(c * rows + r, owned, stride=rows_count), :] = moved_ref[
                    r * sides + j, which, c
                ]
        cols = pl.ds(j * entries, entries)
        both[: 2 * rows, cols], both[2 * rows :, cols] = halves(gathered[...])


def senders_rows(far_flip, near_flip, depth):
    far = lax.axis_index("far")
    near = lax.axis_index("near")
    far = 1 - far if far_flip else far
    near = 1 - near if near_flip else near
    return pl.ds(pl.multiple_of((2 * far + near) * depth, depth), depth)


def products(both, high, low):
    rows = both.shape[0] // 4
    dot = functools.partial(jnp.dot, preferred_element_type=jnp.float32)
    sums = []
    for c in range(2):
        wide = dot(both[...], high[c])
        fine = dot(both[: 2 * rows], low[c])
        sums.append((wide[2 * rows :] + fine) + wide[: 2 * rows])
    real = sums[0][:rows] - sums[1][rows:]
    imag = sums[1][:rows] + sums[0][rows:]
    return real, imag


def most_kernel(early_ref, late_ref, branch_ref, acc_ref, gathered, both):
    depth = both.shape[2]
    step = acc_ref.shape[-1] // STEPS
    senders = [(early_ref, 1, 0, 0), (late_ref, 0, 1, 0), (late_ref, 1, 0, 1)]
    for n, (moved_ref, which, _, _) in enumerate(senders):
        gather(moved_ref, which, gathered, both.at[n])
    for i in range(STEPS):
        cols = pl.ds(i * step, step)
        total = None
        for n, (_, _, *flips) in enumerate(senders):
            part = branch_ref[:, senders_rows(*flips, depth), cols]
            more = products(both.at[n], *halves(part))
            total = more if total is None else (total[0] + more[0], total[1] + more[1])
        acc_ref[0, :, cols], acc_ref[1, :, cols] = total


def last_kernel(moved_ref, branch_ref, prior_ref, out_ref, gathered, both):
    i = pl.program_id(0)

    @pl.when(i == 0)
    def _():
        gather(moved_ref, 0, gathered, both)

    _, owned, rows_count, width = out_ref.shape
    cols = pl.ds(pl.multiple_of(i * width, width), width)
    part = branch_ref[:, senders_rows(1, 1, both.shape[1]), cols]
    real, imag = products(both, *halves(part))
    shape = (owned, rows_count, width)
    out_ref[0] = (prior_ref[0, :, cols] + real).reshape(shape)
    out_ref[1] = (prior_ref[1, :, cols] + imag).reshape(shape)


def absorb_most(early, late, branch):
    blocks, _, _, owned, entries = early.shape
    rows_count = lax.axis_size("row")
    opened = branch.shape[-1]
    rows = owned * rows_count
    depth = blocks // rows_count * entries
    return pl.pallas_call(
        most_kernel,
        in_specs=[whole()] * 3,
        out_specs=whole(),
        out_shape=jax.ShapeDtypeStruct((2, rows, opened), jnp.float32),
        scratch_shapes=[
            pltpu.VMEM((2 * rows, entries), jnp.float32),
            pltpu.VMEM((3, 4 * rows, depth), jnp.bfloat16),
        ],
        compiler_params=params(16),
        name="absorb_most",
    )(early, late, branch)


def absorb_last(moved, branch, prior):
    blocks, _, _, owned, entries = moved.shape
    rows_count = lax.axis_size("row")
    opened = branch.shape[-1]
    rows = owned * rows_count
    depth = blocks // rows_count * entries
    return pl.pallas_call(
        last_kernel,
        grid=(STEPS,),
        in_specs=[whole()] * 3,
        out_specs=pl.BlockSpec(
            (2, owned, rows_count, opened // STEPS), lambda i: (0, 0, 0, i)
        ),
        out_shape=jax.ShapeDtypeStruct((2, owned, rows_count, opened), jnp.float32),
        scratch_shapes=[
            pltpu.VMEM((2 * rows, entries), jnp.float32),
            pltpu.VMEM((4 * rows, depth), jnp.bfloat16),
        ],
        compiler_params=params(16),
        name="absorb_last",
    )(moved, branch, prior)


def over_planes(x, flip):
    count = lax.axis_size("far") * lax.axis_size("near")
    return lax.ppermute(x, ("far", "near"), [(i, i ^ flip) for i in range(count)])


def per_device(stem, branch):
    rows_count, cols_count = counts()
    _, _, entries, remain = stem.shape
    _, contract, opened = branch.shape
    owned = remain // (rows_count * cols_count)
    fits = (
        entries * cols_count == contract
        and rows_count % 2 == 0
        and entries % LANES == 0
        and owned % SUBLANES == 0
        and opened % (STEPS * LANES) == 0
        and remain % (2 * LANES * rows_count) == 0
        and lax.axis_size("far") == lax.axis_size("near") == 2
    )
    if not fits:
        return plain(stem, branch)
    block = (rows_count * lax.axis_size("side"), 2, owned, entries)
    double = (block[0], 2, *block[1:])

    def exchange(x):
        return lax.all_to_all(x, PLANE, split_axis=0, concat_axis=0, tiled=True)

    pairs = [(i, i ^ 1) for i in range(rows_count)]
    branch = lax.ppermute(branch, "row", pairs)
    first, second = small(pack_far_kernel, (stem,), (block,) * 2)
    first = over_planes(first, 2)
    early, beside = small(pack_near_kernel, (stem, second), (double, block))
    beside = over_planes(beside, 1)
    early = exchange(early)
    (second,) = small(part_of_kernel, (early,), (block,))
    second = over_planes(second, 3)
    (late,) = small(join_kernel, (first, beside), (double,))
    late = exchange(late)
    acc = absorb_most(early, late, branch)
    return absorb_last(second[:, None], branch, acc)


def solution(mesh):
    rows_count, cols_count = mesh.shape["row"], mesh.shape["col"]
    parted = Mesh(
        mesh.devices.reshape(rows_count, 2, 2, cols_count // 4), ("row", *COLS)
    )
    return jax.shard_map(
        per_device,
        mesh=parted,
        in_specs=(P(None, "row", COLS, None), P()),
        out_specs=P(None, ("row", *COLS), None, None),
        check_vma=False,
    )
```

```python
import functools

import jax
import jax.numpy as jnp
from jax import lax
from jax.experimental import pallas as pl
from jax.experimental.pallas import tpu as pltpu
from jax.sharding import Mesh, PartitionSpec as P


LANES = 128
SUBLANES = 8
STEPS = 4


COLS = ("far", "near", "side")
PLANE = ("row", "side")


def counts():
    rows_count = lax.axis_size("row")
    cols_count = 1
    for name in COLS:
        cols_count *= lax.axis_size(name)
    return rows_count, cols_count


def plain(stem, branch):
    rows_count, cols_count = counts()
    entries = stem.shape[2]
    remain = stem.shape[3]
    contract = branch.shape[1]
    opened = branch.shape[2]
    middle = entries * cols_count // contract
    owned = remain // (rows_count * cols_count)
    blocks = stem.reshape(2, 1, entries, rows_count * cols_count, owned)
    blocks = jnp.moveaxis(blocks, 3, 0)
    moved = lax.all_to_all(blocks, ("row", *COLS), 0, 0, tiled=True)
    moved = moved.reshape(rows_count, cols_count, 2, entries, owned)
    split = moved.transpose(2, 0, 1, 3, 4).reshape(
        2, rows_count, contract, middle, owned
    )
    high = lax.Precision.HIGHEST
    dot = functools.partial(jnp.einsum, "akml,ko->lamo", precision=high)
    real = dot(split[0], branch[0]) - dot(split[1], branch[1])
    imag = dot(split[0], branch[1]) + dot(split[1], branch[0])
    return jnp.stack([real, imag]).reshape(2, owned, rows_count, middle * opened)


def params(mib):
    return pltpu.CompilerParams(vmem_limit_bytes=mib << 20)


def whole():
    return pl.BlockSpec(memory_space=pltpu.VMEM)


def turned(stem_ref, r, c, width, far):
    start = pl.multiple_of((2 * r + far) * width, width)
    return stem_ref[c, 0, :, pl.ds(start, width)].T


def place(stem_ref, far, same, other):
    entries = stem_ref.shape[2]
    blocks, _, owned, _ = same.shape
    rows_count = lax.axis_size("row")
    sides = blocks // rows_count
    half = sides * owned
    here = lax.axis_index("near") == 0
    for r in range(rows_count):
        at = pl.ds(r * sides, sides)
        for c in range(2):
            whole_width = turned(stem_ref, r, c, 2 * half, far)
            low, high = whole_width[:half], whole_width[half:]
            shape = (sides, owned, entries)
            same[at, c] = jnp.where(here, low, high).reshape(shape)
            other[at, c] = jnp.where(here, high, low).reshape(shape)


def pack_far_kernel(stem_ref, first_ref, second_ref):
    place(stem_ref, 1 - lax.axis_index("far"), first_ref, second_ref)


def mine():
    return lax.axis_index("row") * lax.axis_size("side") + lax.axis_index("side")


def pack_near_kernel(stem_ref, second_ref, *refs):
    *piece_refs, beside_ref, own = refs
    place(stem_ref, lax.axis_index("far"), own, beside_ref)
    for t, piece_ref in enumerate(piece_refs):
        to = jnp.bitwise_xor(mine(), t)
        piece_ref[0] = second_ref[to]
        piece_ref[1] = own[to]


def parts_kernel(first_ref, beside_ref, *piece_refs):
    for t, piece_ref in enumerate(piece_refs):
        to = jnp.bitwise_xor(mine(), t)
        piece_ref[0] = first_ref[to]
        piece_ref[1] = beside_ref[to]


def collect_kernel(*refs):
    *piece_refs, second_ref, own_ref = refs
    for t, piece_ref in enumerate(piece_refs):
        at = jnp.bitwise_xor(mine(), t)
        second_ref[at] = piece_ref[0]
        own_ref[at] = piece_ref[1]


def small(kernel, args, outs, scratch=()):
    return pl.pallas_call(
        kernel,
        in_specs=[whole()] * len(args),
        out_specs=[whole()] * len(outs),
        out_shape=[jax.ShapeDtypeStruct(out, jnp.float32) for out in outs],
        scratch_shapes=[pltpu.VMEM(shape, jnp.float32) for shape in scratch],
        compiler_params=params(4),
    )(*args)


def halves(x):
    high = x.astype(jnp.bfloat16)
    low = (x - high.astype(jnp.float32)).astype(jnp.bfloat16)
    return high, low


def gather(moved_ref, which, gathered, both):
    blocks, _, _, owned, entries = moved_ref.shape
    rows = both.shape[0] // 4
    rows_count = rows // owned
    sides = blocks // rows_count
    for j in range(sides):
        for c in range(2):
            for r in range(rows_count):
                gathered[pl.ds(c * rows + r, owned, stride=rows_count), :] = moved_ref[
                    r * sides + j, which, c
                ]
        cols = pl.ds(j * entries, entries)
        both[: 2 * rows, cols], both[2 * rows :, cols] = halves(gathered[...])


def senders_rows(far_flip, near_flip, depth):
    far = lax.axis_index("far")
    near = lax.axis_index("near")
    far = 1 - far if far_flip else far
    near = 1 - near if near_flip else near
    return pl.ds(pl.multiple_of((2 * far + near) * depth, depth), depth)


def products(both, high, low):
    rows = both.shape[0] // 4
    dot = functools.partial(jnp.dot, preferred_element_type=jnp.float32)
    sums = []
    for c in range(2):
        wide = dot(both[...], high[c])
        fine = dot(both[: 2 * rows], low[c])
        sums.append((wide[2 * rows :] + fine) + wide[: 2 * rows])
    real = sums[0][:rows] - sums[1][rows:]
    imag = sums[1][:rows] + sums[0][rows:]
    return real, imag


def multiply(senders, branch_ref, prior_ref, acc_ref, gathered, both):
    depth = both.shape[2]
    step = acc_ref.shape[-1] // STEPS
    for n, (moved_ref, which, _) in enumerate(senders):
        gather(moved_ref, which, gathered, both.at[n])
    for i in range(STEPS):
        cols = pl.ds(i * step, step)
        total = None
        if prior_ref is not None:
            total = prior_ref[0, :, cols], prior_ref[1, :, cols]
        for n, (_, _, flips) in enumerate(senders):
            part = branch_ref[:, senders_rows(*flips, depth), cols]
            more = products(both.at[n], *halves(part))
            total = more if total is None else (total[0] + more[0], total[1] + more[1])
        acc_ref[0, :, cols], acc_ref[1, :, cols] = total


def own_kernel(own_ref, branch_ref, acc_ref, gathered, both):
    multiply([(own_ref, 0, (0, 0))], branch_ref, None, acc_ref, gathered, both)


def late_kernel(*refs):
    *piece_refs, branch_ref, prior_ref, acc_ref, gathered, both, moved = refs
    for t, piece_ref in enumerate(piece_refs):
        moved[jnp.bitwise_xor(mine(), t)] = piece_ref[...]
    senders = [(moved, 0, (1, 0)), (moved, 1, (0, 1))]
    multiply(senders, branch_ref, prior_ref, acc_ref, gathered, both)


def last_kernel(moved_ref, branch_ref, prior_ref, out_ref, gathered, both):
    i = pl.program_id(0)

    @pl.when(i == 0)
    def _():
        gather(moved_ref, 0, gathered, both)

    _, owned, rows_count, width = out_ref.shape
    cols = pl.ds(pl.multiple_of(i * width, width), width)
    part = branch_ref[:, senders_rows(1, 1, both.shape[1]), cols]
    real, imag = products(both, *halves(part))
    shape = (owned, rows_count, width)
    out_ref[0] = (prior_ref[0, :, cols] + real).reshape(shape)
    out_ref[1] = (prior_ref[1, :, cols] + imag).reshape(shape)


def absorb(kernel, block, args, branch, prior, senders, scratch=()):
    blocks, _, owned, entries = block
    rows_count = lax.axis_size("row")
    opened = branch.shape[-1]
    rows = owned * rows_count
    depth = blocks // rows_count * entries
    args = [*args, branch] + ([] if prior is None else [prior])
    return pl.pallas_call(
        kernel,
        in_specs=[whole()] * len(args),
        out_specs=whole(),
        out_shape=jax.ShapeDtypeStruct((2, rows, opened), jnp.float32),
        scratch_shapes=[
            pltpu.VMEM((2 * rows, entries), jnp.float32),
            pltpu.VMEM((senders, 4 * rows, depth), jnp.bfloat16),
            *(pltpu.VMEM(shape, jnp.float32) for shape in scratch),
        ],
        compiler_params=params(16),
    )(*args)


def absorb_last(moved, branch, prior):
    blocks, _, _, owned, entries = moved.shape
    rows_count = lax.axis_size("row")
    opened = branch.shape[-1]
    rows = owned * rows_count
    depth = blocks // rows_count * entries
    return pl.pallas_call(
        last_kernel,
        grid=(STEPS,),
        in_specs=[whole()] * 3,
        out_specs=pl.BlockSpec(
            (2, owned, rows_count, opened // STEPS), lambda i: (0, 0, 0, i)
        ),
        out_shape=jax.ShapeDtypeStruct((2, owned, rows_count, opened), jnp.float32),
        scratch_shapes=[
            pltpu.VMEM((2 * rows, entries), jnp.float32),
            pltpu.VMEM((4 * rows, depth), jnp.bfloat16),
        ],
        compiler_params=params(16),
        name="absorb_last",
    )(moved, branch, prior)


def over_planes(x, flip):
    count = lax.axis_size("far") * lax.axis_size("near")
    return lax.ppermute(x, ("far", "near"), [(i, i ^ flip) for i in range(count)])


def per_device(stem, branch):
    rows_count, cols_count = counts()
    _, _, entries, remain = stem.shape
    _, contract, opened = branch.shape
    owned = remain // (rows_count * cols_count)
    plane = rows_count * lax.axis_size("side")
    fits = (
        entries * cols_count == contract
        and rows_count % 2 == 0
        and plane & (plane - 1) == 0
        and entries % LANES == 0
        and owned % SUBLANES == 0
        and opened % (STEPS * LANES) == 0
        and remain % (2 * LANES * rows_count) == 0
        and lax.axis_size("far") == lax.axis_size("near") == 2
    )
    if not fits:
        return plain(stem, branch)
    block = (plane, 2, owned, entries)
    piece = (2, *block[1:])

    def exchange(pieces):
        moved = list(pieces)
        for t in range(plane - 1, 0, -1):
            pairs = [(i, i ^ t) for i in range(plane)]
            moved[t] = lax.ppermute(pieces[t], PLANE, pairs)
        return moved

    pairs = [(i, i ^ 1) for i in range(rows_count)]
    branch = lax.ppermute(branch, "row", pairs)
    first, second = small(pack_far_kernel, (stem,), (block,) * 2)
    first = over_planes(first, 2)
    *early, beside = small(
        pack_near_kernel, (stem, second), (piece,) * plane + (block,), (block,)
    )
    beside = over_planes(beside, 1)
    early = exchange(early)
    second, own = small(collect_kernel, early, (block,) * 2)
    second = over_planes(second, 3)
    late = small(parts_kernel, (first, beside), (piece,) * plane)
    late = exchange(late)
    acc = absorb(own_kernel, block, [own[:, None]], branch, None, 1)
    moved = (plane, *piece)
    acc = absorb(late_kernel, block, late, branch, acc, 2, (moved,))
    return absorb_last(second[:, None], branch, acc)


def solution(mesh):
    rows_count, cols_count = mesh.shape["row"], mesh.shape["col"]
    parted = Mesh(
        mesh.devices.reshape(rows_count, 2, 2, cols_count // 4), ("row", *COLS)
    )
    return jax.shard_map(
        per_device,
        mesh=parted,
        in_specs=(P(None, "row", COLS, None), P()),
        out_specs=P(None, ("row", *COLS), None, None),
        check_vma=False,
    )
```

```python
import functools

import jax
import jax.numpy as jnp
from jax import lax
from jax.experimental import pallas as pl
from jax.experimental.pallas import tpu as pltpu
from jax.sharding import Mesh, PartitionSpec as P


LANES = 128
SUBLANES = 8
STEPS = 4


COLS = ("far", "near", "side")
PLANE = ("row", "side")


def counts():
    rows_count = lax.axis_size("row")
    cols_count = 1
    for name in COLS:
        cols_count *= lax.axis_size(name)
    return rows_count, cols_count


def plain(stem, branch):
    rows_count, cols_count = counts()
    entries = stem.shape[2]
    remain = stem.shape[3]
    contract = branch.shape[1]
    opened = branch.shape[2]
    middle = entries * cols_count // contract
    owned = remain // (rows_count * cols_count)
    blocks = stem.reshape(2, 1, entries, rows_count * cols_count, owned)
    blocks = jnp.moveaxis(blocks, 3, 0)
    moved = lax.all_to_all(blocks, ("row", *COLS), 0, 0, tiled=True)
    moved = moved.reshape(rows_count, cols_count, 2, entries, owned)
    split = moved.transpose(2, 0, 1, 3, 4).reshape(
        2, rows_count, contract, middle, owned
    )
    high = lax.Precision.HIGHEST
    dot = functools.partial(jnp.einsum, "akml,ko->lamo", precision=high)
    real = dot(split[0], branch[0]) - dot(split[1], branch[1])
    imag = dot(split[0], branch[1]) + dot(split[1], branch[0])
    return jnp.stack([real, imag]).reshape(2, owned, rows_count, middle * opened)


def params(mib):
    return pltpu.CompilerParams(vmem_limit_bytes=mib << 20)


def whole():
    return pl.BlockSpec(memory_space=pltpu.VMEM)


def turned(stem_ref, r, c, width, far):
    start = pl.multiple_of((2 * r + far) * width, width)
    return stem_ref[c, 0, :, pl.ds(start, width)].T


def place(stem_ref, far, same, other):
    entries = stem_ref.shape[2]
    blocks, _, owned, _ = same.shape
    rows_count = lax.axis_size("row")
    sides = blocks // rows_count
    half = sides * owned
    here = lax.axis_index("near") == 0
    for r in range(rows_count):
        at = pl.ds(r * sides, sides)
        for c in range(2):
            whole_width = turned(stem_ref, r, c, 2 * half, far)
            low, high = whole_width[:half], whole_width[half:]
            shape = (sides, owned, entries)
            same[at, c] = jnp.where(here, low, high).reshape(shape)
            other[at, c] = jnp.where(here, high, low).reshape(shape)


def pack_far_kernel(stem_ref, first_ref, second_ref):
    place(stem_ref, 1 - lax.axis_index("far"), first_ref, second_ref)


def mine():
    return lax.axis_index("row") * lax.axis_size("side") + lax.axis_index("side")


def pack_near_kernel(stem_ref, second_ref, *refs):
    *piece_refs, beside_ref, own = refs
    place(stem_ref, lax.axis_index("far"), own, beside_ref)
    for t, piece_ref in enumerate(piece_refs):
        to = jnp.bitwise_xor(mine(), t)
        piece_ref[0] = second_ref[to]
        piece_ref[1] = own[to]


def parts_kernel(first_ref, beside_ref, *piece_refs):
    for t, piece_ref in enumerate(piece_refs):
        to = jnp.bitwise_xor(mine(), t)
        piece_ref[0] = first_ref[to]
        piece_ref[1] = beside_ref[to]


def collect_kernel(*refs):
    *piece_refs, second_ref, own_ref = refs
    for t, piece_ref in enumerate(piece_refs):
        at = jnp.bitwise_xor(mine(), t)
        second_ref[at] = piece_ref[0]
        own_ref[at] = piece_ref[1]


def small(kernel, args, outs, scratch=()):
    return pl.pallas_call(
        kernel,
        in_specs=[whole()] * len(args),
        out_specs=[whole()] * len(outs),
        out_shape=[jax.ShapeDtypeStruct(out, jnp.float32) for out in outs],
        scratch_shapes=[pltpu.VMEM(shape, jnp.float32) for shape in scratch],
        compiler_params=params(4),
    )(*args)


def halves(x):
    high = x.astype(jnp.bfloat16)
    low = (x - high.astype(jnp.float32)).astype(jnp.bfloat16)
    return high, low


def gather(moved_ref, which, gathered, both):
    blocks, _, _, owned, entries = moved_ref.shape
    rows = both.shape[0] // 4
    rows_count = rows // owned
    sides = blocks // rows_count
    for j in range(sides):
        for c in range(2):
            for r in range(rows_count):
                gathered[pl.ds(c * rows + r, owned, stride=rows_count), :] = moved_ref[
                    r * sides + j, which, c
                ]
        cols = pl.ds(j * entries, entries)
        both[: 2 * rows, cols], both[2 * rows :, cols] = halves(gathered[...])


def senders_rows(far_flip, near_flip, depth):
    far = lax.axis_index("far")
    near = lax.axis_index("near")
    far = 1 - far if far_flip else far
    near = 1 - near if near_flip else near
    return pl.ds(pl.multiple_of((2 * far + near) * depth, depth), depth)


def products(both, high, low):
    rows = both.shape[0] // 4
    dot = functools.partial(jnp.dot, preferred_element_type=jnp.float32)
    sums = []
    for c in range(2):
        wide = dot(both[...], high[c])
        fine = dot(both[: 2 * rows], low[c])
        sums.append((wide[2 * rows :] + fine) + wide[: 2 * rows])
    real = sums[0][:rows] - sums[1][rows:]
    imag = sums[1][:rows] + sums[0][rows:]
    return real, imag


def multiply(senders, branch_ref, prior_ref, acc_ref, gathered, both):
    depth = both.shape[2]
    step = acc_ref.shape[-1] // STEPS
    for n, (moved_ref, which, _) in enumerate(senders):
        gather(moved_ref, which, gathered, both.at[n])
    for i in range(STEPS):
        cols = pl.ds(i * step, step)
        total = None
        if prior_ref is not None:
            total = prior_ref[0, :, cols], prior_ref[1, :, cols]
        for n, (_, _, flips) in enumerate(senders):
            part = branch_ref[:, senders_rows(*flips, depth), cols]
            more = products(both.at[n], *halves(part))
            total = more if total is None else (total[0] + more[0], total[1] + more[1])
        acc_ref[0, :, cols], acc_ref[1, :, cols] = total


def own_kernel(own_ref, branch_ref, acc_ref, gathered, both):
    multiply([(own_ref, 0, (0, 0))], branch_ref, None, acc_ref, gathered, both)


def late_kernel(*refs):
    *piece_refs, branch_ref, prior_ref, acc_ref, gathered, both, moved = refs
    for t, piece_ref in enumerate(piece_refs):
        moved[jnp.bitwise_xor(mine(), t)] = piece_ref[...]
    senders = [(moved, 0, (1, 0)), (moved, 1, (0, 1))]
    multiply(senders, branch_ref, prior_ref, acc_ref, gathered, both)


def last_kernel(
    moved_ref, branch_ref, prior_ref, out_ref, gathered, both, result, sems
):
    gather(moved_ref, 0, gathered, both)
    _, owned, rows_count, opened = result.shape
    step = opened // STEPS
    copies = []
    for i in range(STEPS):
        cols = pl.ds(i * step, step)
        part = branch_ref[:, senders_rows(1, 1, both.shape[1]), cols]
        real, imag = products(both, *halves(part))
        shape = (owned, rows_count, step)
        result[0, :, :, cols] = (prior_ref[0, :, cols] + real).reshape(shape)
        result[1, :, :, cols] = (prior_ref[1, :, cols] + imag).reshape(shape)
        copies.append(
            pltpu.make_async_copy(
                result.at[:, :, :, cols], out_ref.at[:, :, :, cols], sems.at[i]
            )
        )
        copies[-1].start()
    for copy in copies:
        copy.wait()


def absorb(kernel, block, args, branch, prior, senders, scratch=()):
    blocks, _, owned, entries = block
    rows_count = lax.axis_size("row")
    opened = branch.shape[-1]
    rows = owned * rows_count
    depth = blocks // rows_count * entries
    args = [*args, branch] + ([] if prior is None else [prior])
    return pl.pallas_call(
        kernel,
        in_specs=[whole()] * len(args),
        out_specs=whole(),
        out_shape=jax.ShapeDtypeStruct((2, rows, opened), jnp.float32),
        scratch_shapes=[
            pltpu.VMEM((2 * rows, entries), jnp.float32),
            pltpu.VMEM((senders, 4 * rows, depth), jnp.bfloat16),
            *(pltpu.VMEM(shape, jnp.float32) for shape in scratch),
        ],
        compiler_params=params(16),
    )(*args)


def absorb_last(moved, branch, prior):
    blocks, _, _, owned, entries = moved.shape
    rows_count = lax.axis_size("row")
    opened = branch.shape[-1]
    rows = owned * rows_count
    depth = blocks // rows_count * entries
    out = (2, owned, rows_count, opened)
    return pl.pallas_call(
        last_kernel,
        in_specs=[whole()] * 3,
        out_specs=pl.BlockSpec(memory_space=pl.ANY),
        out_shape=jax.ShapeDtypeStruct(out, jnp.float32),
        scratch_shapes=[
            pltpu.VMEM((2 * rows, entries), jnp.float32),
            pltpu.VMEM((4 * rows, depth), jnp.bfloat16),
            pltpu.VMEM(out, jnp.float32),
            pltpu.SemaphoreType.DMA((STEPS,)),
        ],
        compiler_params=params(16),
        name="absorb_last",
    )(moved, branch, prior)


def over_planes(x, flip):
    count = lax.axis_size("far") * lax.axis_size("near")
    return lax.ppermute(x, ("far", "near"), [(i, i ^ flip) for i in range(count)])


def turns(plane, sides):
    def key(t):
        side, core, chip = t % sides, t // sides % 2, t // (2 * sides)
        return side == 0, side == chip == 0, core, -chip, -side

    return sorted(range(1, plane), key=key)


def per_device(stem, branch):
    rows_count, cols_count = counts()
    _, _, entries, remain = stem.shape
    _, contract, opened = branch.shape
    owned = remain // (rows_count * cols_count)
    plane = rows_count * lax.axis_size("side")
    fits = (
        entries * cols_count == contract
        and rows_count % 2 == 0
        and plane & (plane - 1) == 0
        and entries % LANES == 0
        and owned % SUBLANES == 0
        and opened % (STEPS * LANES) == 0
        and remain % (2 * LANES * rows_count) == 0
        and lax.axis_size("far") == lax.axis_size("near") == 2
    )
    if not fits:
        return plain(stem, branch)
    block = (plane, 2, owned, entries)
    piece = (2, *block[1:])

    def exchange(pieces):
        moved = list(pieces)
        for t in turns(plane, lax.axis_size("side")):
            pairs = [(i, i ^ t) for i in range(plane)]
            moved[t] = lax.ppermute(pieces[t], PLANE, pairs)
        return moved

    pairs = [(i, i) for i in range(rows_count)]
    branch = lax.ppermute(branch, "row", pairs)
    first, second = small(pack_far_kernel, (stem,), (block,) * 2)
    first = over_planes(first, 2)
    *early, beside = small(
        pack_near_kernel, (stem, second), (piece,) * plane + (block,), (block,)
    )
    beside = over_planes(beside, 1)
    early = exchange(early)
    second, own = small(collect_kernel, early, (block,) * 2)
    second = over_planes(second, 3)
    late = small(parts_kernel, (first, beside), (piece,) * plane)
    late = exchange(late)
    acc = absorb(own_kernel, block, [own[:, None]], branch, None, 1)
    moved = (plane, *piece)
    acc = absorb(late_kernel, block, late, branch, acc, 2, (moved,))
    return absorb_last(second[:, None], branch, acc)


def solution(mesh):
    rows_count, cols_count = mesh.shape["row"], mesh.shape["col"]
    parted = Mesh(
        mesh.devices.reshape(rows_count, 2, 2, cols_count // 4), ("row", *COLS)
    )
    return jax.shard_map(
        per_device,
        mesh=parted,
        in_specs=(P(None, "row", COLS, None), P()),
        out_specs=P(None, ("row", *COLS), None, None),
        check_vma=False,
    )
```

```python
import functools

import jax
import jax.numpy as jnp
from jax import lax
from jax.experimental import pallas as pl
from jax.experimental.pallas import tpu as pltpu
from jax.sharding import Mesh, PartitionSpec as P


LANES = 128
SUBLANES = 8
STEPS = 4


COLS = ("far", "near", "side")
PLANE = ("row", "side")


def counts():
    rows_count = lax.axis_size("row")
    cols_count = 1
    for name in COLS:
        cols_count *= lax.axis_size(name)
    return rows_count, cols_count


def plain(stem, branch):
    rows_count, cols_count = counts()
    entries = stem.shape[2]
    remain = stem.shape[3]
    contract = branch.shape[1]
    opened = branch.shape[2]
    middle = entries * cols_count // contract
    owned = remain // (rows_count * cols_count)
    blocks = stem.reshape(2, 1, entries, rows_count * cols_count, owned)
    blocks = jnp.moveaxis(blocks, 3, 0)
    moved = lax.all_to_all(blocks, ("row", *COLS), 0, 0, tiled=True)
    moved = moved.reshape(rows_count, cols_count, 2, entries, owned)
    split = moved.transpose(2, 0, 1, 3, 4).reshape(
        2, rows_count, contract, middle, owned
    )
    high = lax.Precision.HIGHEST
    dot = functools.partial(jnp.einsum, "akml,ko->lamo", precision=high)
    real = dot(split[0], branch[0]) - dot(split[1], branch[1])
    imag = dot(split[0], branch[1]) + dot(split[1], branch[0])
    return jnp.stack([real, imag]).reshape(2, owned, rows_count, middle * opened)


def params(mib):
    return pltpu.CompilerParams(vmem_limit_bytes=mib << 20)


def whole():
    return pl.BlockSpec(memory_space=pltpu.VMEM)


def turned(stem_ref, r, c, width, far):
    start = pl.multiple_of((2 * r + far) * width, width)
    return stem_ref[c, 0, :, pl.ds(start, width)].T


def place(stem_ref, far, same, other):
    entries = stem_ref.shape[2]
    blocks, _, owned, _ = same.shape
    rows_count = lax.axis_size("row")
    sides = blocks // rows_count
    half = sides * owned
    here = lax.axis_index("near") == 0
    for r in range(rows_count):
        at = pl.ds(r * sides, sides)
        for c in range(2):
            whole_width = turned(stem_ref, r, c, 2 * half, far)
            low, high = whole_width[:half], whole_width[half:]
            shape = (sides, owned, entries)
            same[at, c] = jnp.where(here, low, high).reshape(shape)
            other[at, c] = jnp.where(here, high, low).reshape(shape)


def pack_far_kernel(stem_ref, first_ref, second_ref):
    place(stem_ref, 1 - lax.axis_index("far"), first_ref, second_ref)


def mine():
    return lax.axis_index("row") * lax.axis_size("side") + lax.axis_index("side")


def pack_near_kernel(stem_ref, second_ref, *refs):
    *piece_refs, beside_ref, own = refs
    place(stem_ref, lax.axis_index("far"), own, beside_ref)
    for t, piece_ref in enumerate(piece_refs):
        to = jnp.bitwise_xor(mine(), t)
        piece_ref[0] = second_ref[to]
        piece_ref[1] = own[to]


def parts_kernel(first_ref, beside_ref, *piece_refs):
    for t, piece_ref in enumerate(piece_refs):
        to = jnp.bitwise_xor(mine(), t)
        piece_ref[0] = first_ref[to]
        piece_ref[1] = beside_ref[to]


def collect_kernel(*refs):
    *piece_refs, second_ref, own_ref = refs
    for t, piece_ref in enumerate(piece_refs):
        at = jnp.bitwise_xor(mine(), t)
        second_ref[at] = piece_ref[0]
        own_ref[at] = piece_ref[1]


def small(kernel, args, outs, scratch=()):
    return pl.pallas_call(
        kernel,
        in_specs=[whole()] * len(args),
        out_specs=[whole()] * len(outs),
        out_shape=[jax.ShapeDtypeStruct(out, jnp.float32) for out in outs],
        scratch_shapes=[pltpu.VMEM(shape, jnp.float32) for shape in scratch],
        compiler_params=params(4),
    )(*args)


def halves(x):
    high = x.astype(jnp.bfloat16)
    low = (x - high.astype(jnp.float32)).astype(jnp.bfloat16)
    return high, low


def gather(moved_ref, which, gathered, both):
    blocks, _, _, owned, entries = moved_ref.shape
    rows = both.shape[0] // 4
    rows_count = rows // owned
    sides = blocks // rows_count
    for j in range(sides):
        for c in range(2):
            for r in range(rows_count):
                gathered[pl.ds(c * rows + r, owned, stride=rows_count), :] = moved_ref[
                    r * sides + j, which, c
                ]
        cols = pl.ds(j * entries, entries)
        both[: 2 * rows, cols], both[2 * rows :, cols] = halves(gathered[...])


def senders_rows(far_flip, near_flip, depth):
    far = lax.axis_index("far")
    near = lax.axis_index("near")
    far = 1 - far if far_flip else far
    near = 1 - near if near_flip else near
    return pl.ds(pl.multiple_of((2 * far + near) * depth, depth), depth)


def products(both, high, low):
    rows = both.shape[0] // 4
    dot = functools.partial(jnp.dot, preferred_element_type=jnp.float32)
    sums = []
    for c in range(2):
        wide = dot(both[...], high[c])
        fine = dot(both[: 2 * rows], low[c])
        sums.append((wide[2 * rows :] + fine) + wide[: 2 * rows])
    real = sums[0][:rows] - sums[1][rows:]
    imag = sums[1][:rows] + sums[0][rows:]
    return real, imag


def multiply(senders, branch_ref, prior_ref, acc_ref, gathered, both):
    depth = both.shape[2]
    step = acc_ref.shape[-1] // STEPS
    for n, (moved_ref, which, _) in enumerate(senders):
        gather(moved_ref, which, gathered, both.at[n])
    for i in range(STEPS):
        cols = pl.ds(i * step, step)
        total = None
        if prior_ref is not None:
            total = prior_ref[0, :, cols], prior_ref[1, :, cols]
        for n, (_, _, flips) in enumerate(senders):
            part = branch_ref[:, senders_rows(*flips, depth), cols]
            more = products(both.at[n], *halves(part))
            total = more if total is None else (total[0] + more[0], total[1] + more[1])
        acc_ref[0, :, cols], acc_ref[1, :, cols] = total


def own_kernel(own_ref, branch_ref, acc_ref, gathered, both):
    multiply([(own_ref, 0, (0, 0))], branch_ref, None, acc_ref, gathered, both)


def late_kernel(group, *refs):
    *piece_refs, branch_ref, prior_ref, acc_ref, gathered, both, moved = refs
    rows_count, _, _, owned, entries = moved.shape
    rows = rows_count * owned
    sides = lax.axis_size("side")
    for n, piece_ref in enumerate(piece_refs):
        moved[jnp.bitwise_xor(lax.axis_index("row"), n)] = piece_ref[...]
    far, near = lax.axis_index("far"), lax.axis_index("near")
    side = jnp.bitwise_xor(lax.axis_index("side"), group)
    places = (2 * (1 - far) + near, 2 * far + 1 - near)
    starts = [
        pl.multiple_of((place_ * sides + side) * entries, entries) for place_ in places
    ]
    for which in range(2):
        for c in range(2):
            for r in range(rows_count):
                gathered[pl.ds(c * rows + r, owned, stride=rows_count), :] = moved[
                    r, which, c
                ]
        cols = pl.ds(which * entries, entries)
        both[: 2 * rows, cols], both[2 * rows :, cols] = halves(gathered[...])
    step = acc_ref.shape[-1] // STEPS
    for i in range(STEPS):
        cols = pl.ds(i * step, step)
        parts = [halves(branch_ref[:, pl.ds(start, entries), cols]) for start in starts]
        high, low = (jnp.concatenate(part, axis=1) for part in zip(*parts))
        real, imag = products(both, high, low)
        acc_ref[0, :, cols] = prior_ref[0, :, cols] + real
        acc_ref[1, :, cols] = prior_ref[1, :, cols] + imag


def last_kernel(
    moved_ref, branch_ref, prior_ref, out_ref, gathered, both, result, sems
):
    gather(moved_ref, 0, gathered, both)
    _, owned, rows_count, opened = result.shape
    step = opened // STEPS
    copies = []
    for i in range(STEPS):
        cols = pl.ds(i * step, step)
        part = branch_ref[:, senders_rows(1, 1, both.shape[1]), cols]
        real, imag = products(both, *halves(part))
        shape = (owned, rows_count, step)
        result[0, :, :, cols] = (prior_ref[0, :, cols] + real).reshape(shape)
        result[1, :, :, cols] = (prior_ref[1, :, cols] + imag).reshape(shape)
        copies.append(
            pltpu.make_async_copy(
                result.at[:, :, :, cols], out_ref.at[:, :, :, cols], sems.at[i]
            )
        )
        copies[-1].start()
    for copy in copies:
        copy.wait()


def absorb(kernel, block, args, branch, prior, both, scratch=()):
    _, _, owned, entries = block
    rows_count = lax.axis_size("row")
    opened = branch.shape[-1]
    rows = owned * rows_count
    args = [*args, branch] + ([] if prior is None else [prior])
    return pl.pallas_call(
        kernel,
        in_specs=[whole()] * len(args),
        out_specs=whole(),
        out_shape=jax.ShapeDtypeStruct((2, rows, opened), jnp.float32),
        scratch_shapes=[
            pltpu.VMEM((2 * rows, entries), jnp.float32),
            pltpu.VMEM(both, jnp.bfloat16),
            *(pltpu.VMEM(shape, jnp.float32) for shape in scratch),
        ],
        compiler_params=params(16),
    )(*args)


def absorb_last(moved, branch, prior):
    blocks, _, _, owned, entries = moved.shape
    rows_count = lax.axis_size("row")
    opened = branch.shape[-1]
    rows = owned * rows_count
    depth = blocks // rows_count * entries
    out = (2, owned, rows_count, opened)
    return pl.pallas_call(
        last_kernel,
        in_specs=[whole()] * 3,
        out_specs=pl.BlockSpec(memory_space=pl.ANY),
        out_shape=jax.ShapeDtypeStruct(out, jnp.float32),
        scratch_shapes=[
            pltpu.VMEM((2 * rows, entries), jnp.float32),
            pltpu.VMEM((4 * rows, depth), jnp.bfloat16),
            pltpu.VMEM(out, jnp.float32),
            pltpu.SemaphoreType.DMA((STEPS,)),
        ],
        compiler_params=params(16),
        name="absorb_last",
    )(moved, branch, prior)


def over_planes(x, flip):
    count = lax.axis_size("far") * lax.axis_size("near")
    return lax.ppermute(x, ("far", "near"), [(i, i ^ flip) for i in range(count)])


def turns(plane, sides):
    def key(t):
        side, core, chip = t % sides, t // sides % 2, t // (2 * sides)
        return 5 * (side == 0) + 4 * core + 2 * (chip == 0), -chip, -side

    return sorted(range(1, plane), key=key)


def per_device(stem, branch):
    rows_count, cols_count = counts()
    _, _, entries, remain = stem.shape
    _, contract, opened = branch.shape
    owned = remain // (rows_count * cols_count)
    plane = rows_count * lax.axis_size("side")
    fits = (
        entries * cols_count == contract
        and rows_count % 2 == 0
        and plane & (plane - 1) == 0
        and entries % LANES == 0
        and owned % SUBLANES == 0
        and opened % (STEPS * LANES) == 0
        and remain % (2 * LANES * rows_count) == 0
        and lax.axis_size("far") == lax.axis_size("near") == 2
    )
    if not fits:
        return plain(stem, branch)
    block = (plane, 2, owned, entries)
    piece = (2, *block[1:])

    def exchange(pieces):
        moved = list(pieces)
        for t in turns(plane, lax.axis_size("side")):
            pairs = [(i, i ^ t) for i in range(plane)]
            moved[t] = lax.ppermute(pieces[t], PLANE, pairs)
        return moved

    pairs = [(i, i) for i in range(rows_count)]
    branch = lax.ppermute(branch, "row", pairs)
    first, second = small(pack_far_kernel, (stem,), (block,) * 2)
    first = over_planes(first, 2)
    *early, beside = small(
        pack_near_kernel, (stem, second), (piece,) * plane + (block,), (block,)
    )
    beside = over_planes(beside, 1)
    early = exchange(early)
    second, own = small(collect_kernel, early, (block,) * 2)
    second = over_planes(second, 3)
    late = small(parts_kernel, (first, beside), (piece,) * plane)
    late = exchange(late)
    sides = lax.axis_size("side")
    rows = 4 * owned * rows_count
    both = (1, rows, sides * entries)
    acc = absorb(own_kernel, block, [own[:, None]], branch, None, both)
    for group in range(sides - 1, -1, -1):
        acc = absorb(
            functools.partial(late_kernel, group),
            block,
            late[group::sides],
            branch,
            acc,
            (rows, 2 * entries),
            ((rows_count, *piece),),
        )
    return absorb_last(second[:, None], branch, acc)


def solution(mesh):
    rows_count, cols_count = mesh.shape["row"], mesh.shape["col"]
    parted = Mesh(
        mesh.devices.reshape(rows_count, 2, 2, cols_count // 4), ("row", *COLS)
    )
    return jax.shard_map(
        per_device,
        mesh=parted,
        in_specs=(P(None, "row", COLS, None), P()),
        out_specs=P(None, ("row", *COLS), None, None),
        check_vma=False,
    )
```
